32 devices in a mesh: grp: 2 (over core), row: 4 (over y, x), col: 4 (over z).
Axes of the slice: x: 2, y: 2, z: 4, core: 2. Of those that a mesh axis runs over, the one named last changes fastest.
Arguments:
- front: float32 [16384, 16384], P(('grp', 'row'), 'col'), may hold values from -9 to 1400, as said below
- prev_lower: bfloat16 [16384, 256], P(('grp', 'row', 'col')), may hold values from -0.035888672 to 0.035888672
- prev_pivots: float32 [256], replicated, may hold values from 150 to 400
- pivot_order: int32 [2, 256], replicated, may hold values from 0 to 255, each once within a row
Outputs:
- schur: float32 [16384, 16384], P(('grp', 'row'), 'col')
- panels_scaled: float32 [16384, 512], P(('grp', 'row', 'col'))
- pivots: float32 [512], replicated
The draws below stay inside these ranges and needn't reach their ends.
Inputs may be any that keep to these rules, and one draw needn't show every extreme that they name: front is symmetric and positive definite, and stays so after the update by the pending panel, so that every Schur complement of the window is positive definite. Each row of pivot_order names every number of 0 to 255 once.
All inputs are finite; a program needn't handle non-finite values.
Results may differ from the reference program's by a relative error of at most 0.0003.
Values may be sent and summed in bfloat16 or wider, within the bound.
A program may use at most 192 MiB of HBM per device.

```python
import math
import jax
import jax.numpy as jnp
from jax import lax

R = 16384
PB = 256
STEPS = 2


def draw_front(key, part):
    leading, second = jax.random.split(key, 2)
    entries = jnp.clip(jax.random.normal(leading, (R, R), jnp.float32), -6.0, 6.0)
    symmetric = (entries + entries.T) * 0.70710678
    diag_values = jax.random.uniform(second, (R,), jnp.float32, 400.0, 700.0)
    positions = jnp.arange(R, dtype=jnp.int32)
    symmetric = symmetric.at[positions, positions].set(diag_values)
    return symmetric


def steps_of(rng, extent, pieces, least, high):
    loudness, own = 1.0, jax.random.fold_in(rng, 6)
    for position, parts in pieces:
        heights = jnp.exp(jax.random.uniform(jax.random.fold_in(own, position), (parts,), jnp.float32, least / len(pieces), high / len(pieces)))
        loudness = loudness * jnp.repeat(heights, extent[position] // parts).reshape([-1 if axis == position else 1 for axis in range(len(extent))])
    return loudness


def bell_draw(rng, shape, deviation, bound, pieces=(), kind=jnp.bfloat16):
    array = deviation * jax.random.normal(rng, shape, jnp.float32)
    if pieces:
        array = array * steps_of(rng, shape, pieces, -0.22, 0.18)
    return jnp.clip(array, -bound, bound).astype(kind)


def setup_inputs(seed: int = 0) -> dict:
    key_list = jax.random.split(jax.random.key(seed), 5)
    return {
        "front": draw_front(jax.random.fold_in(key_list[4], 71), 0),
        "prev_lower": bell_draw(key_list[1], (R, PB), (0.096 * PB ** -0.5), 0.035888672, ((0, 32),)),
        "prev_pivots": jnp.clip(jnp.exp(jax.random.uniform(key_list[2], (PB,), jnp.float32, math.log(150.0), math.log(400.0))), 150.0, 400.0),
        "pivot_order": jax.vmap(lambda own: jax.random.permutation(own, PB))(jax.random.split(key_list[3], STEPS)).reshape((STEPS, PB)).astype(jnp.int32),
    }


def apply_panel(matrix, factor_rows, pivot_values):
    exact = lax.Precision.HIGHEST
    scaled = (factor_rows.astype(jnp.float32) * pivot_values).astype(jnp.bfloat16)
    return matrix - jnp.dot(scaled.astype(jnp.float32), factor_rows.astype(jnp.float32).T, precision=exact)

def reference(front, prev_lower, prev_pivots, pivot_order):
    exact = lax.Precision.HIGHEST
    panel_width = prev_lower.shape[1]
    panel_count = pivot_order.shape[0]
    row_ids = jnp.arange(front.shape[0], dtype=jnp.int32)
    matrix = front
    factor_rows = prev_lower
    pivot_values = prev_pivots
    outputs = []
    pivot_list = []
    for panel_index in range(panel_count):
        matrix = apply_panel(matrix, factor_rows, pivot_values)
        start = panel_index * panel_width
        panel_cols = matrix[:, start:start + panel_width]
        select = (pivot_order[panel_index][:, None] == jnp.arange(panel_width, dtype=jnp.int32)[None, :]).astype(jnp.float32)
        diagonal_block = panel_cols[start:start + panel_width]
        permuted = jnp.dot(jnp.dot(select, diagonal_block, precision=exact), select.T, precision=exact)
        cholesky_factor = jnp.linalg.cholesky(permuted)
        root_diag = jnp.diagonal(cholesky_factor)
        moved = jnp.dot(panel_cols, select.T, precision=exact)
        solved = lax.linalg.triangular_solve(cholesky_factor, moved, left_side=False, lower=True, transpose_a=True)
        live_rows = (row_ids >= start)[:, None]
        shown_rows = jnp.where(live_rows, solved / root_diag, jnp.zeros_like(solved)).astype(jnp.bfloat16)
        pivot_values = root_diag * root_diag
        outputs.append(shown_rows.astype(jnp.float32) * pivot_values)
        pivot_list.append(pivot_values)
        trailing_rows = (row_ids >= start + panel_width)[:, None]
        factor_rows = jnp.where(trailing_rows, shown_rows, jnp.zeros_like(shown_rows))
    return (matrix, jnp.concatenate(outputs, axis=1), jnp.concatenate(pivot_list))
```

```python
import jax
import jax.numpy as jnp
from jax import lax
from jax.sharding import PartitionSpec as P

EVERY = ("grp", "row", "col")
EXACT = lax.Precision.HIGHEST


def scale(factor_rows, pivot_values):
    return (factor_rows.astype(jnp.float32) * pivot_values).astype(jnp.bfloat16)


def outer(scaled, factor_cols):
    return lax.dot_general(
        scaled, factor_cols, (((1,), (1,)), ((), ())), preferred_element_type=jnp.float32
    )


def send_from_first(array):
    grp, row, col = (lax.axis_size(axis) for axis in EVERY)
    reached = [(0, 0, 0)]

    def level(array, moves):
        pairs = []
        for source, target in moves:
            pairs.append(
                tuple((g * row + r) * col + c for g, r, c in (source, target))
            )
            reached.append(target)
        return array + lax.ppermute(array, EVERY, pairs)

    for axis, size in ((1, row), (2, col), (0, grp)):
        span = 1
        while span * 2 < size:
            span *= 2
        while span >= 1:
            moves = []
            for place in list(reached):
                to = place[axis] + span
                target = place[:axis] + (to,) + place[axis + 1 :]
                if to < size and target not in reached:
                    moves.append((place, target))
            array = level(array, moves)
            span //= 2
    return array


def scatter_over_col(rows, own_rows):
    col = lax.axis_size("col")
    part = jnp.where(lax.axis_index("col") == 0, rows[:own_rows], jnp.zeros_like(rows[:own_rows]))
    for target in range(1, col):
        piece = rows[target * own_rows : (target + 1) * own_rows]
        part = part + lax.ppermute(piece, "col", [(0, target)])
    return part


def gather_rows(part):
    return lax.all_gather(part, "col", axis=0, tiled=True)


def gather_cols(part):
    row_devices = lax.axis_size("grp") * lax.axis_size("row")
    col_devices = lax.axis_size("col")
    pairs = [
        (number, (number % row_devices) * col_devices + number // row_devices)
        for number in range(row_devices * col_devices)
    ]
    moved = lax.ppermute(part, EVERY, pairs)
    return lax.all_gather(moved, ("grp", "row"), axis=0, tiled=True)


def body(front, prev_lower, prev_pivots, pivot_order):
    row_count, col_count = front.shape
    own_rows, width = prev_lower.shape
    panel_count = pivot_order.shape[0]
    span = panel_count * width
    row_block = lax.axis_index("grp") * lax.axis_size("row") + lax.axis_index("row")
    col_block = lax.axis_index("col")
    rows_here = row_block * row_count + jnp.arange(row_count, dtype=jnp.int32)
    own_here = row_block * row_count + col_block * own_rows + jnp.arange(own_rows, dtype=jnp.int32)
    first = (row_block == 0) & (col_block == 0)

    prev_rows = gather_rows(prev_lower)
    prev_cols = gather_cols(prev_lower)
    lead = prev_lower[:span] if own_rows >= span else prev_rows[:span]
    corner = front[:span, :span] - outer(scale(lead, prev_pivots), lead)
    corner = jnp.where(first, corner, jnp.zeros_like(corner))
    blocks = [
        send_from_first(corner[k * width : (k + 1) * width, : (k + 1) * width])
        for k in range(panel_count)
    ]

    row_scaled = [scale(prev_rows, prev_pivots)]
    row_final = [row_scaled[0]]
    col_lower = [prev_cols]
    lead_lower = [prev_cols[:span]]
    outputs = []
    pivot_list = []
    for index in range(panel_count):
        start, end = index * width, (index + 1) * width
        panel = front[:, start:end] - outer(
            jnp.concatenate(row_scaled, axis=1),
            jnp.concatenate([lower[start:end] for lower in lead_lower], axis=1),
        )
        below = [blocks[k][:, start:end] for k in range(index + 1, panel_count)]
        pivot_row = pivot_order[index]
        select = (pivot_row[:, None] == jnp.arange(width, dtype=jnp.int32)[None, :]).astype(
            jnp.float32
        )
        diagonal = blocks[index][:, start:end]
        permuted = jnp.dot(jnp.dot(select, diagonal, precision=EXACT), select.T, precision=EXACT)
        cholesky_factor = jnp.linalg.cholesky(permuted)
        root_diag = jnp.diagonal(cholesky_factor)
        pivot_values = root_diag * root_diag
        moved = jnp.dot(jnp.concatenate([panel] + below, axis=0), select.T, precision=EXACT)
        solved = lax.linalg.triangular_solve(
            cholesky_factor, moved, left_side=False, lower=True, transpose_a=True
        )
        factor = (solved / root_diag).astype(jnp.bfloat16)
        rows = factor[:row_count]
        part = scatter_over_col(
            jnp.where((rows_here >= start)[:, None], rows, jnp.zeros_like(rows)), own_rows
        )
        outputs.append(part.astype(jnp.float32) * pivot_values)
        pivot_list.append(pivot_values)
        if index + 1 < panel_count:
            live = jnp.where((own_here >= end)[:, None], part, jnp.zeros_like(part))
            col_lower.append(gather_cols(live))
            own_block = jnp.where((rows_here >= end)[:, None], rows, jnp.zeros_like(rows))
            row_scaled.append(scale(own_block, pivot_values))
            tail = factor[row_count:]
            lead_lower.append(
                jnp.concatenate([jnp.zeros((end, width), tail.dtype), tail], axis=0)
            )
            tail_scaled = scale(tail, pivot_values)
            for k in range(index + 1, panel_count):
                at = (k - index - 1) * width
                change = outer(tail_scaled[at : at + width], tail[: at + width])
                blocks[k] = blocks[k].at[:, end:].add(-change)
            row_final.append(scale(gather_rows(live), pivot_values))
    schur = front - outer(
        jnp.concatenate(row_final, axis=1), jnp.concatenate(col_lower, axis=1)
    )
    return (schur, jnp.concatenate(outputs, axis=1), jnp.concatenate(pivot_list))


def solution(mesh):
    in_specs = (P(("grp", "row"), "col"), P(("grp", "row", "col"), None), P(), P())
    out_specs = (P(("grp", "row"), "col"), P(("grp", "row", "col"), None), P())
    return jax.shard_map(body, mesh=mesh, in_specs=in_specs, out_specs=out_specs, check_vma=False)
```
